256 devices in a mesh: cohort: 4 (over x, y), tile: 64 (over z, core).
Axes of the slice: x: 2, y: 2, z: 32, core: 2. Of those that a mesh axis runs over, the one named last changes fastest.
The devices are a block of a 4x8x32 slice.
Arguments:
- dosage: bfloat16 [4096, 8192], P(('cohort', 'tile')), parts along dimension 0, may hold values from 0 to 2
- covars: float32 [4096, 16], P(('cohort', 'tile')), parts along dimension 0, may hold values from -12 to 12, as said below
- phenotypes: float32 [4096, 7168], P(('cohort', 'tile')), parts along dimension 0, may hold values from -100 to 100
Outputs:
- mean_chi: float32 [28672], P(('cohort', 'tile')), parts along dimension 0
- hit_rate: float32 [28672], P(('cohort', 'tile')), parts along dimension 0
The draws below stay inside these ranges and needn't reach their ends.
There are 4 independent parts, one for each index of `cohort`. The reference program is written for one: setup_inputs(seed, part) draws one part's arguments, and reference() takes and returns one part's arrays. A program takes and returns all parts, laid end to end along the dimension named above; each array names one. Nothing has to cross between parts.
Inputs may be any that keep to these rules, and one draw needn't show every extreme that they name: `covars`: each covariate column has its own mean and spread.
All inputs are finite; a program needn't handle non-finite values.
Results may differ from the reference program's by a relative error of at most 0.003.
Values may be sent and summed in bfloat16 or wider, within the bound.
No kernel may reach another device: no remote copies, remote signals or barrier semaphores. Data moves between devices by JAX's collectives and lax.ppermute only.
A program may use at most 64 MiB of HBM per device.

```python
import math
import jax
import jax.numpy as jnp
from jax import lax

VARIANTS = 8192
COVS = 16
SAMPLES = 1024
GENES = 7168


def ancestry_score(key):
    label = (jax.random.uniform(jax.random.fold_in(key, 14), (SAMPLES,), jnp.float32) < 0.4).astype(jnp.float32)
    blur = jnp.clip(jax.random.normal(jax.random.fold_in(key, 15), (SAMPLES,), jnp.float32), -4.0, 4.0)
    return label + 0.15 * blur


def covar_table(key):
    base = jnp.clip(jax.random.normal(jax.random.fold_in(key, 11), (SAMPLES, COVS), jnp.float32), -5.0, 5.0)
    score = 2.0 * ancestry_score(key) - 1.0
    base = jnp.concatenate([score[:, None], base[:, 1:]], axis=1)
    means = jax.random.uniform(jax.random.fold_in(key, 12), (COVS,), jnp.float32, -2.0, 2.0)
    spread = jnp.exp(jax.random.uniform(jax.random.fold_in(key, 13), (COVS,), jnp.float32, math.log(0.5), math.log(2.0)))
    return base * spread[None, :] + means[None, :]


def draw_covars(key, part):
    return covar_table(key)


def draw_dosage(key, part):
    score = ancestry_score(key)
    base_freq = jax.random.uniform(jax.random.fold_in(key, 31), (VARIANTS,), jnp.float32, 0.05, 0.95)
    shift = jax.random.uniform(jax.random.fold_in(key, 32), (VARIANTS,), jnp.float32, -0.4, 0.4)
    freq = jnp.clip(base_freq[None, :] + shift[None, :] * (score[:, None] - 0.5), 0.02, 0.98)
    first = (jax.random.uniform(jax.random.fold_in(key, 33), (SAMPLES, VARIANTS), jnp.float32) < freq).astype(jnp.float32)
    second = (jax.random.uniform(jax.random.fold_in(key, 34), (SAMPLES, VARIANTS), jnp.float32) < freq).astype(jnp.float32)
    blur = 0.2 * jnp.clip(jax.random.normal(jax.random.fold_in(key, 35), (SAMPLES, VARIANTS), jnp.float32), -3.0, 3.0)
    return jnp.clip(first + second + blur, 0.0, 2.0).astype(jnp.bfloat16)


def draw_phenotypes(key, part):
    table = covar_table(key)
    effect = jnp.clip(jax.random.normal(jax.random.fold_in(key, 21), (COVS, GENES), jnp.float32), -4.0, 4.0)
    spread = jnp.exp(jax.random.uniform(jax.random.fold_in(key, 22), (GENES,), jnp.float32, math.log(0.5), math.log(2.0)))
    noise = jnp.clip(jax.random.normal(jax.random.fold_in(key, 23), (SAMPLES, GENES), jnp.float32), -8.0, 8.0) * spread[None, :]
    signal = jnp.dot(table, effect, precision=lax.Precision.HIGHEST)
    return jnp.clip(signal + noise, -100.0, 100.0)


def setup_inputs(seed: int = 0, part: int = 0) -> dict:
    streams_of = jax.random.split(jax.random.key(seed), 4)
    own_keys = jax.random.split(jax.random.fold_in(streams_of[3], part), 4)
    dosage = draw_dosage(jax.random.fold_in(jax.random.fold_in(streams_of[3], part), 71), part)
    covars = draw_covars(jax.random.fold_in(jax.random.fold_in(streams_of[3], part), 71), part)
    phenotypes = draw_phenotypes(jax.random.fold_in(jax.random.fold_in(streams_of[3], part), 71), part)
    return dict(dosage=dosage, covars=covars, phenotypes=phenotypes)


def reference(dosage, covars, phenotypes):
    highest = lax.Precision.HIGHEST
    dose_real = dosage.astype(jnp.float32)
    samples = dose_real.shape[0]
    variants = dose_real.shape[1]
    gram = jnp.dot(covars.T.astype(jnp.float32), covars.astype(jnp.float32), precision=highest, preferred_element_type=jnp.float32)
    cov_dose = jnp.dot(covars.T.astype(jnp.float32), dose_real.astype(jnp.float32), precision=highest, preferred_element_type=jnp.float32)
    cov_pheno = jnp.dot(covars.T.astype(jnp.float32), phenotypes.astype(jnp.float32), precision=highest, preferred_element_type=jnp.float32)
    factor = jnp.linalg.cholesky(gram)
    betas = jax.scipy.linalg.cho_solve((factor, True), jnp.concatenate([cov_dose, cov_pheno], axis=1))
    beta_dose = betas[:, :variants]
    beta_pheno = betas[:, variants:]
    dose_resid = dose_real - jnp.dot(covars.astype(jnp.float32), beta_dose.astype(jnp.float32), precision=highest, preferred_element_type=jnp.float32)
    pheno_resid = phenotypes - jnp.dot(covars.astype(jnp.float32), beta_pheno.astype(jnp.float32), precision=highest, preferred_element_type=jnp.float32)
    dose_sumsq = lax.optimization_barrier(jnp.sum(dose_resid * dose_resid, axis=0))
    pheno_sumsq = lax.optimization_barrier(jnp.sum(pheno_resid * pheno_resid, axis=0))
    dose_bf = dose_resid.astype(jnp.bfloat16)
    pheno_bf = pheno_resid.astype(jnp.bfloat16)
    cross = lax.dot_general(pheno_bf.astype(jnp.float32), dose_bf.astype(jnp.float32), (((0,), (0,)), ((), ())), preferred_element_type=jnp.float32)
    dose_var = dose_sumsq / samples + 0.1
    pheno_var = pheno_sumsq / samples + 0.1
    zscore = cross / (jnp.sqrt(jnp.float32(samples)) * jnp.sqrt(pheno_var[:, None] * dose_var[None, :]))
    chi_square = zscore * zscore
    mean_chi = lax.optimization_barrier(jnp.mean(chi_square, axis=1))
    hit_rate = 20.0 / variants * lax.optimization_barrier(jnp.sum(jax.nn.sigmoid(2.0 * (chi_square - 4.0)), axis=1))
    return (mean_chi, hit_rate)
```

```python
import functools

import jax
import jax.numpy as jnp
from jax import lax
from jax.experimental import pallas as pl
from jax.experimental.pallas import tpu as pltpu
from jax.sharding import Mesh
from jax.sharding import PartitionSpec as P


CORES = 2
PARTS = 2
SWAPS = (4, 8, 12, 15)
STAGES = (3, 4, 5, 6, 7)
ABSORBS = (9, 11, 14)
VMEM_LIMIT = 24 << 20
WIDTH = 512
LANES = 128
VARIANCE_FLOOR = 0.1
HIGHEST = lax.Precision.HIGHEST
AXES = ("cohort", "z", "core")
TILE = ("z", "core")
SWAP = [(0, 1), (1, 0)]


def dot(a, b, dims):
    return lax.dot_general(
        a, b, ((dims[0], dims[1]), ((), ())), precision=HIGHEST, preferred_element_type=jnp.float32
    )


def orthonormal(table):
    gram = dot(table, table, ((0,), (0,)))
    factor = jnp.linalg.cholesky(gram)
    inverse = lax.linalg.triangular_solve(
        factor, jnp.eye(gram.shape[0], dtype=jnp.float32), left_side=True, lower=True
    )
    return dot(table, inverse, ((1,), (1,)))


def split(x, parts):
    terms = []
    for _ in range(parts):
        term = lax.reduce_precision(x, 8, 7)
        terms.append(term.astype(jnp.bfloat16))
        x = x - term
    return terms


def products(genes, covs, left, dose):
    both = jnp.dot(left, dose, preferred_element_type=jnp.float32)
    base = 2 * genes
    along = both[base : base + covs] + both[base + covs : base + 2 * covs]
    along = along + both[base + 2 * covs : base + 3 * covs]
    real = dose.astype(jnp.float32)
    return both[:genes] + both[genes:base], along, jnp.sum(real * real, axis=0, keepdims=True)


def group_sums(genes, covs, part, left_ref, pieces, before, at):
    rows = pieces[-1].shape[0] // PARTS
    dose = [piece[:, at] for piece in pieces[:-1]] + [pieces[-1][part * rows : (part + 1) * rows, at]]
    dose = jnp.concatenate(dose, axis=0)
    values = products(genes, covs, left_ref[...], dose)
    return tuple(x + ref[:, at] for x, ref in zip(values, before)) if before else values


def absorb(genes, covs, part, count, left_ref, *refs):
    pieces, before, after = refs[:count], refs[count:-3], refs[-3:]

    @pl.loop(0, pieces[0].shape[1] // WIDTH)
    def _(i):
        at = pl.ds(pl.multiple_of(i * WIDTH, WIDTH), WIDTH)
        for ref, value in zip(after, group_sums(genes, covs, part, left_ref, pieces, before, at)):
            ref[:, at] = value


def finish(samples, genes, covs, part, count, left_ref, *refs):
    pieces, before, (chi_ref, hit_ref) = refs[:count], refs[count:-2], refs[-2:]

    def step(i, totals):
        chi_total, hit_total = totals
        at = pl.ds(pl.multiple_of(i * WIDTH, WIDTH), WIDTH)
        cross, along, square = group_sums(genes, covs, part, left_ref, pieces, before, at)
        sumsq = square - jnp.sum(along * along, axis=0, keepdims=True)
        variance = jnp.maximum(sumsq, 0.0) / samples + VARIANCE_FLOOR
        zscore = cross * lax.rsqrt(variance * samples)
        chi = zscore * zscore
        hit = 1.0 / (1.0 + jnp.exp(8.0 - 2.0 * chi))
        for k in range(WIDTH // LANES):
            chi_total = chi_total + chi[:, k * LANES : (k + 1) * LANES]
            hit_total = hit_total + hit[:, k * LANES : (k + 1) * LANES]
        return chi_total, hit_total

    zeros = jnp.zeros((genes, LANES), jnp.float32)
    chi_ref[...], hit_ref[...] = lax.fori_loop(0, pieces[0].shape[1] // WIDTH, step, (zeros, zeros))


def call(body, shapes, left, pieces, before):
    vmem = pl.BlockSpec(memory_space=pltpu.VMEM)
    operands = [left, *pieces, *before]
    size = left.shape[1] * pieces[0].shape[1]
    return pl.pallas_call(
        functools.partial(body, len(pieces)),
        out_shape=tuple(jax.ShapeDtypeStruct(s, jnp.float32) for s in shapes),
        in_specs=[vmem] * len(operands),
        out_specs=(vmem,) * len(shapes),
        compiler_params=pltpu.CompilerParams(vmem_limit_bytes=VMEM_LIMIT),
        cost_estimate=pl.CostEstimate(flops=2 * left.shape[0] * size, bytes_accessed=2 * size, transcendentals=0),
    )(*operands)


def lay(*refs):
    start = 0
    for ref in refs[:-1]:
        refs[-1][start : start + ref.shape[0], :] = ref[...]
        start += ref.shape[0]


def packed_rows(pieces):
    vmem = pl.BlockSpec(memory_space=pltpu.VMEM)
    rows, width = sum(x.shape[0] for x in pieces), pieces[0].shape[1]
    return pl.pallas_call(
        lay,
        out_shape=jax.ShapeDtypeStruct((rows, width), pieces[0].dtype),
        in_specs=[vmem] * len(pieces),
        out_specs=vmem,
        compiler_params=pltpu.CompilerParams(vmem_limit_bytes=VMEM_LIMIT),
        cost_estimate=pl.CostEstimate(flops=rows * width, bytes_accessed=4 * rows * width, transcendentals=0),
    )(*pieces)


def groups(reach):
    edges = [0, *SWAPS]
    spans = list(zip(edges, edges[1:]))
    return [
        (range(a, reach + 1 if b == SWAPS[-1] else b), range(a + 1, b + 1)) for a, b in spans
    ]


def paired(packed, core):
    chips, rows, _, width = packed.shape
    first = core == 0
    mine = lax.dynamic_index_in_dim(packed, core, 2, keepdims=False)
    give = lax.dynamic_index_in_dim(packed, 1 - core, 2, keepdims=False)
    take = lax.ppermute(give, "core", SWAP)
    packed = jnp.stack([jnp.where(first, mine, take), jnp.where(first, take, mine)], axis=1)
    return packed.reshape(chips * CORES * rows, width)


def residuals(basis, pheno):
    resid = pheno - dot(basis, dot(basis, pheno, ((0,), (0,))), ((1,), (0,)))
    variance = jnp.mean(resid * resid, axis=0) + VARIANCE_FLOOR
    return jnp.stack(split(resid * lax.rsqrt(variance)[None, :], 2))


def assembled(basis, terms, z, core):
    others = lax.ppermute(terms, "core", SWAP)
    chips = lax.axis_size("z")
    sign = 1 - 2 * core
    order = []
    for keeps, gives in groups(chips // 2):
        order += [z - sign * k for k in keeps] + [z + sign * k for k in gives]
    order = lax.rem(jnp.stack(order) + chips, chips)

    def laid(x):
        count, samples, width = x.shape
        x = x.reshape(count, chips, samples // chips, width)[:, order].reshape(x.shape)
        return x.transpose(0, 2, 1).reshape(count * width, samples)

    return jnp.concatenate(
        [laid(jnp.stack([terms[0], others[0], terms[1], others[1]])), laid(jnp.stack(split(basis, 3)))], axis=0
    )


def local(dosage, covars, phenotypes):
    chips = lax.axis_size("z")
    devices = chips * CORES
    rows, variants = dosage.shape
    covs = covars.shape[1]
    samples = rows * devices
    own = phenotypes.shape[1] // devices
    z = lax.axis_index("z")
    core = lax.axis_index("core")
    first = core == 0
    half = variants // CORES
    reach = chips // 2

    travel = [(2 * i, 2 * ((i + 1) % chips)) for i in range(chips)]
    travel += [(2 * i + 1, 2 * ((i - 1) % chips) + 1) for i in range(chips)]

    theirs = lax.ppermute(dosage, "core", SWAP)
    block = jnp.concatenate([jnp.where(first, dosage, theirs), jnp.where(first, theirs, dosage)], axis=0)
    part = half // PARTS
    keep = jnp.where(first, block[:, :half], block[:, half:])
    give = jnp.where(first, block[:, half:], block[:, :half])
    keep = [keep[:, i * part : (i + 1) * part] for i in range(PARTS)]
    give = [give[:, i * part : (i + 1) * part] for i in range(PARTS)]

    packed = jnp.concatenate(
        [
            phenotypes.reshape(rows, chips, CORES, own),
            jnp.broadcast_to(covars[:, None, None, :], (rows, chips, CORES, covs)),
        ],
        axis=3,
    ).reshape(rows, chips, CORES * (own + covs))
    packed = lax.all_to_all(packed, "z", split_axis=1, concat_axis=0, tiled=True)
    packed = packed.reshape(chips, rows, CORES, own + covs)

    kept, given = [keep], []
    swapped = []
    partial = [()] * PARTS
    genes = 2 * own

    def absorbed(index):
        keeps, gives = groups(reach)[index]
        size = (len(keeps) + len(gives)) * CORES * rows
        start = sum(len(x) + len(y) for x, y in groups(reach)[:index]) * CORES * rows
        used = left[:, start : start + size]
        last = index == len(SWAPS) - 1
        shapes = [(genes, LANES)] * 2 if last else [(genes, part), (covs, part), (1, part)]
        body = functools.partial(finish, samples) if last else absorb
        return [
            call(functools.partial(body, genes, covs, i), shapes, used, [kept[k][i] for k in keeps] + [swapped[index]], x)
            for i, x in enumerate(partial)
        ]

    for step in range(1, reach):
        held = give[-1]
        moved = []
        for value in keep + give:
            moved.append(lax.ppermute(value, TILE, travel))
        keep, give = moved[:PARTS], moved[PARTS:]
        kept.append(list(keep))
        given.append(give)
        if step in STAGES:
            packed, held = lax.optimization_barrier((packed, held))
        if step == STAGES[0]:
            keep[0], packed = lax.optimization_barrier((keep[0], paired(packed, core)))
        if step == STAGES[1]:
            keep[0], basis = lax.optimization_barrier((keep[0], orthonormal(packed[:, own:])))
        if step == STAGES[2]:
            keep[0], basis = lax.optimization_barrier((keep[0], orthonormal(basis)))
        if step == STAGES[3]:
            keep[0], terms = lax.optimization_barrier((keep[0], residuals(basis, packed[:, :own])))
        if step == STAGES[4]:
            keep[0], left = lax.optimization_barrier((keep[0], assembled(basis, terms, z, core)))
        if step in SWAPS:
            rows_given = packed_rows([x for y in zip(*given) for x in y])
            swapped.append(lax.ppermute(rows_given, "core", SWAP))
            given = []
        if step in ABSORBS:
            partial = absorbed(ABSORBS.index(step))
    for i, value in enumerate(keep):
        keep[i] = lax.ppermute(value, TILE, travel)
    kept.append(keep)
    chi, hit = (x + y for x, y in zip(*absorbed(len(SWAPS) - 1)))
    sums = jnp.stack([jnp.sum(chi, axis=1), jnp.sum(hit, axis=1)])
    sums = sums[:, :own] + lax.ppermute(sums[:, own:], "core", SWAP)
    return (sums[0] / variants, 20.0 / variants * sums[1])


def solution(mesh):
    cohorts, tiles = mesh.shape["cohort"], mesh.shape["tile"]
    finer = Mesh(mesh.devices.reshape(cohorts, tiles // CORES, CORES), AXES)
    return jax.shard_map(
        local,
        mesh=finer,
        in_specs=(P(AXES, None), P(AXES, None), P(AXES, None)),
        out_specs=(P(AXES), P(AXES)),
        check_vma=False,
    )
```

```python
import functools

import jax
import jax.numpy as jnp
from jax import lax
from jax.experimental import pallas as pl
from jax.experimental.pallas import tpu as pltpu
from jax.sharding import Mesh
from jax.sharding import PartitionSpec as P


CORES = 2
PARTS = 1
SWAPS = (5, 10, 15)
STAGES = (3, 4, 5, 6, 7)
ABSORBS = (9, 13)
VMEM_LIMIT = 24 << 20
WIDTH = 512
LANES = 128
VARIANCE_FLOOR = 0.1
HIGHEST = lax.Precision.HIGHEST
AXES = ("cohort", "z", "core")
TILE = ("z", "core")
SWAP = [(0, 1), (1, 0)]


def dot(a, b, dims):
    return lax.dot_general(
        a, b, ((dims[0], dims[1]), ((), ())), precision=HIGHEST, preferred_element_type=jnp.float32
    )


def orthonormal(table):
    gram = dot(table, table, ((0,), (0,)))
    factor = jnp.linalg.cholesky(gram)
    inverse = lax.linalg.triangular_solve(
        factor, jnp.eye(gram.shape[0], dtype=jnp.float32), left_side=True, lower=True
    )
    return dot(table, inverse, ((1,), (1,)))


def split(x, parts):
    terms = []
    for _ in range(parts):
        term = lax.reduce_precision(x, 8, 7)
        terms.append(term.astype(jnp.bfloat16))
        x = x - term
    return terms


def products(genes, covs, left, dose):
    both = jnp.dot(left, dose, preferred_element_type=jnp.float32)
    base = 2 * genes
    along = both[base : base + covs] + both[base + covs : base + 2 * covs]
    along = along + both[base + 2 * covs : base + 3 * covs]
    real = dose.astype(jnp.float32)
    return both[:genes] + both[genes:base], along, jnp.sum(real * real, axis=0, keepdims=True)


def group_sums(genes, covs, part, left_ref, pieces, before, at):
    rows = pieces[-1].shape[0] // PARTS
    dose = [piece[:, at] for piece in pieces[:-1]] + [pieces[-1][part * rows : (part + 1) * rows, at]]
    dose = jnp.concatenate(dose, axis=0)
    values = products(genes, covs, left_ref[...], dose)
    return tuple(x + ref[:, at] for x, ref in zip(values, before)) if before else values


def absorb(genes, covs, part, count, left_ref, *refs):
    pieces, before, after = refs[:count], refs[count:-3], refs[-3:]

    @pl.loop(0, pieces[0].shape[1] // WIDTH)
    def _(i):
        at = pl.ds(pl.multiple_of(i * WIDTH, WIDTH), WIDTH)
        for ref, value in zip(after, group_sums(genes, covs, part, left_ref, pieces, before, at)):
            ref[:, at] = value


def finish(samples, genes, covs, part, count, left_ref, *refs):
    pieces, before, (chi_ref, hit_ref) = refs[:count], refs[count:-2], refs[-2:]

    def step(i, totals):
        chi_total, hit_total = totals
        at = pl.ds(pl.multiple_of(i * WIDTH, WIDTH), WIDTH)
        cross, along, square = group_sums(genes, covs, part, left_ref, pieces, before, at)
        sumsq = square - jnp.sum(along * along, axis=0, keepdims=True)
        variance = jnp.maximum(sumsq, 0.0) / samples + VARIANCE_FLOOR
        zscore = cross * lax.rsqrt(variance * samples)
        chi = zscore * zscore
        hit = 1.0 / (1.0 + jnp.exp(8.0 - 2.0 * chi))
        for k in range(WIDTH // LANES):
            chi_total = chi_total + chi[:, k * LANES : (k + 1) * LANES]
            hit_total = hit_total + hit[:, k * LANES : (k + 1) * LANES]
        return chi_total, hit_total

    zeros = jnp.zeros((genes, LANES), jnp.float32)
    chi_ref[...], hit_ref[...] = lax.fori_loop(0, pieces[0].shape[1] // WIDTH, step, (zeros, zeros))


def call(body, shapes, left, pieces, before):
    vmem = pl.BlockSpec(memory_space=pltpu.VMEM)
    operands = [left, *pieces, *before]
    size = left.shape[1] * pieces[0].shape[1]
    return pl.pallas_call(
        functools.partial(body, len(pieces)),
        out_shape=tuple(jax.ShapeDtypeStruct(s, jnp.float32) for s in shapes),
        in_specs=[vmem] * len(operands),
        out_specs=(vmem,) * len(shapes),
        compiler_params=pltpu.CompilerParams(vmem_limit_bytes=VMEM_LIMIT),
        cost_estimate=pl.CostEstimate(flops=2 * left.shape[0] * size, bytes_accessed=2 * size, transcendentals=0),
    )(*operands)


def lay(*refs):
    start = 0
    for ref in refs[:-1]:
        refs[-1][start : start + ref.shape[0], :] = ref[...]
        start += ref.shape[0]


def packed_rows(pieces):
    vmem = pl.BlockSpec(memory_space=pltpu.VMEM)
    rows, width = sum(x.shape[0] for x in pieces), pieces[0].shape[1]
    return pl.pallas_call(
        lay,
        out_shape=jax.ShapeDtypeStruct((rows, width), pieces[0].dtype),
        in_specs=[vmem] * len(pieces),
        out_specs=vmem,
        compiler_params=pltpu.CompilerParams(vmem_limit_bytes=VMEM_LIMIT),
        cost_estimate=pl.CostEstimate(flops=rows * width, bytes_accessed=4 * rows * width, transcendentals=0),
    )(*pieces)


def groups(reach):
    edges = [0, *SWAPS]
    spans = list(zip(edges, edges[1:]))
    return [
        (range(a, reach + 1 if b == SWAPS[-1] else b), range(a + 1, b + 1)) for a, b in spans
    ]


def offsets(chips):
    order = []
    for keeps, gives in groups(chips // 2):
        order += [-k % chips for k in keeps] + [k % chips for k in gives]
    return order


def ordered(packed, z, core):
    chips, rows, _, width = packed.shape
    first = core == 0
    mine = lax.dynamic_index_in_dim(packed, core, 2, keepdims=False)
    give = lax.dynamic_index_in_dim(packed, 1 - core, 2, keepdims=False)
    take = lax.ppermute(give, "core", SWAP)
    packed = jnp.stack([jnp.where(first, mine, take), jnp.where(first, take, mine)], axis=1)
    sign = 1 - 2 * core
    order = lax.rem(jnp.stack([z + sign * k for k in offsets(chips)]) + chips, chips)
    return packed.reshape(chips, CORES * rows, width)[order].reshape(chips * CORES * rows, width)


def turn(chips, value_ref, out_ref):
    rows = value_ref.shape[0] // chips
    order = offsets(chips)
    for i, k in enumerate(order):
        j = order.index(-k % chips)
        out_ref[i * rows : (i + 1) * rows, :] = value_ref[j * rows : (j + 1) * rows, :]


def turned(value, chips):
    vmem = pl.BlockSpec(memory_space=pltpu.VMEM)
    return pl.pallas_call(
        functools.partial(turn, chips),
        out_shape=jax.ShapeDtypeStruct(value.shape, value.dtype),
        in_specs=[vmem],
        out_specs=vmem,
        compiler_params=pltpu.CompilerParams(vmem_limit_bytes=VMEM_LIMIT),
        cost_estimate=pl.CostEstimate(flops=value.size, bytes_accessed=8 * value.size, transcendentals=0),
    )(value)


def residuals(basis, pheno, chips):
    resid = pheno - dot(basis, dot(basis, pheno, ((0,), (0,))), ((1,), (0,)))
    variance = jnp.mean(resid * resid, axis=0) + VARIANCE_FLOOR
    scaled = resid * lax.rsqrt(variance)[None, :]
    return jnp.stack(split(scaled.T, 2)), jnp.stack(split(turned(scaled, chips).T, 2))


def assembled(basis, terms):
    mine, sent = terms
    others = lax.ppermute(sent, "core", SWAP)
    return jnp.concatenate([mine[0], others[0], mine[1], others[1]] + split(basis.T, 3), axis=0)


def local(dosage, covars, phenotypes):
    chips = lax.axis_size("z")
    devices = chips * CORES
    rows, variants = dosage.shape
    covs = covars.shape[1]
    samples = rows * devices
    own = phenotypes.shape[1] // devices
    z = lax.axis_index("z")
    core = lax.axis_index("core")
    first = core == 0
    half = variants // CORES
    reach = chips // 2

    travel = [(2 * i, 2 * ((i + 1) % chips)) for i in range(chips)]
    travel += [(2 * i + 1, 2 * ((i - 1) % chips) + 1) for i in range(chips)]

    theirs = lax.ppermute(dosage, "core", SWAP)
    block = jnp.concatenate([jnp.where(first, dosage, theirs), jnp.where(first, theirs, dosage)], axis=0)
    part = half // PARTS
    keep = jnp.where(first, block[:, :half], block[:, half:])
    give = jnp.where(first, block[:, half:], block[:, :half])
    keep = [keep[:, i * part : (i + 1) * part] for i in range(PARTS)]
    give = [give[:, i * part : (i + 1) * part] for i in range(PARTS)]

    packed = jnp.concatenate(
        [
            phenotypes.reshape(rows, chips, CORES, own),
            jnp.broadcast_to(covars[:, None, None, :], (rows, chips, CORES, covs)),
        ],
        axis=3,
    ).reshape(rows, chips, CORES * (own + covs))
    packed = lax.all_to_all(packed, "z", split_axis=1, concat_axis=0, tiled=True)
    packed = packed.reshape(chips, rows, CORES, own + covs)

    kept, given = [keep], []
    swapped = []
    partial = [()] * PARTS
    genes = 2 * own

    def absorbed(index):
        keeps, gives = groups(reach)[index]
        size = (len(keeps) + len(gives)) * CORES * rows
        start = sum(len(x) + len(y) for x, y in groups(reach)[:index]) * CORES * rows
        used = left[:, start : start + size]
        last = index == len(SWAPS) - 1
        shapes = [(genes, LANES)] * 2 if last else [(genes, part), (covs, part), (1, part)]
        body = functools.partial(finish, samples) if last else absorb
        return [
            call(functools.partial(body, genes, covs, i), shapes, used, [kept[k][i] for k in keeps] + [swapped[index]], x)
            for i, x in enumerate(partial)
        ]

    for step in range(1, reach):
        held = give[-1]
        moved = []
        for value in keep + give:
            moved.append(lax.ppermute(value, TILE, travel))
        keep, give = moved[:PARTS], moved[PARTS:]
        kept.append(list(keep))
        given.append(give)
        if step in STAGES:
            packed, held = lax.optimization_barrier((packed, held))
        if step == STAGES[0]:
            keep[0], packed = lax.optimization_barrier((keep[0], ordered(packed, z, core)))
        if step == STAGES[1]:
            keep[0], basis = lax.optimization_barrier((keep[0], orthonormal(packed[:, own:])))
        if step == STAGES[2]:
            keep[0], basis = lax.optimization_barrier((keep[0], orthonormal(basis)))
        if step == STAGES[3]:
            keep[0], terms = lax.optimization_barrier((keep[0], residuals(basis, packed[:, :own], chips)))
        if step == STAGES[4]:
            keep[0], left = lax.optimization_barrier((keep[0], assembled(basis, terms)))
        if step in SWAPS:
            rows_given = packed_rows([x for y in zip(*given) for x in y])
            swapped.append(lax.ppermute(rows_given, "core", SWAP))
            given = []
        if step in ABSORBS:
            partial = absorbed(ABSORBS.index(step))
    for i, value in enumerate(keep):
        keep[i] = lax.ppermute(value, TILE, travel)
    kept.append(keep)
    chi, hit = (sum(x) for x in zip(*absorbed(len(SWAPS) - 1)))
    sums = jnp.stack([jnp.sum(chi, axis=1), jnp.sum(hit, axis=1)])
    sums = sums[:, :own] + lax.ppermute(sums[:, own:], "core", SWAP)
    return (sums[0] / variants, 20.0 / variants * sums[1])


def solution(mesh):
    cohorts, tiles = mesh.shape["cohort"], mesh.shape["tile"]
    finer = Mesh(mesh.devices.reshape(cohorts, tiles // CORES, CORES), AXES)
    return jax.shard_map(
        local,
        mesh=finer,
        in_specs=(P(AXES, None), P(AXES, None), P(AXES, None)),
        out_specs=(P(AXES), P(AXES)),
        check_vma=False,
    )
```

```python
import functools

import jax
import jax.numpy as jnp
from jax import lax
from jax.experimental import pallas as pl
from jax.experimental.pallas import tpu as pltpu
from jax.sharding import Mesh
from jax.sharding import PartitionSpec as P


CORES = 2
PARTS = 1
SWAPS = (6, 12, 15)
STAGES = (3, 4, 5, 6, 7)
ABSORBS = (9, 14)
VMEM_LIMIT = 24 << 20
WIDTH = 512
LANES = 128
VARIANCE_FLOOR = 0.1
HIGHEST = lax.Precision.HIGHEST
AXES = ("cohort", "z", "core")
TILE = ("z", "core")
SWAP = [(0, 1), (1, 0)]


def dot(a, b, dims):
    return lax.dot_general(
        a, b, ((dims[0], dims[1]), ((), ())), precision=HIGHEST, preferred_element_type=jnp.float32
    )


def orthonormal(table):
    gram = dot(table, table, ((0,), (0,)))
    factor = jnp.linalg.cholesky(gram)
    inverse = lax.linalg.triangular_solve(
        factor, jnp.eye(gram.shape[0], dtype=jnp.float32), left_side=True, lower=True
    )
    return dot(table, inverse, ((1,), (1,)))


def split(x, parts):
    terms = []
    for _ in range(parts):
        term = lax.reduce_precision(x, 8, 7)
        terms.append(term.astype(jnp.bfloat16))
        x = x - term
    return terms


def products(genes, covs, left, dose):
    both = jnp.dot(left, dose, preferred_element_type=jnp.float32)
    base = 2 * genes
    along = both[base : base + covs] + both[base + covs : base + 2 * covs]
    along = along + both[base + 2 * covs : base + 3 * covs]
    real = dose.astype(jnp.float32)
    return both[:genes] + both[genes:base], along, jnp.sum(real * real, axis=0, keepdims=True)


def group_sums(genes, covs, part, left_ref, pieces, before, at):
    rows = pieces[-1].shape[0] // PARTS
    dose = [piece[:, at] for piece in pieces[:-1]] + [pieces[-1][part * rows : (part + 1) * rows, at]]
    dose = jnp.concatenate(dose, axis=0)
    values = products(genes, covs, left_ref[...], dose)
    return tuple(x + ref[:, at] for x, ref in zip(values, before)) if before else values


def absorb(genes, covs, part, count, left_ref, *refs):
    pieces, before, after = refs[:count], refs[count:-3], refs[-3:]

    @pl.loop(0, pieces[0].shape[1] // WIDTH)
    def _(i):
        at = pl.ds(pl.multiple_of(i * WIDTH, WIDTH), WIDTH)
        for ref, value in zip(after, group_sums(genes, covs, part, left_ref, pieces, before, at)):
            ref[:, at] = value


def finish(samples, genes, covs, part, count, left_ref, *refs):
    pieces, before, (chi_ref, hit_ref) = refs[:count], refs[count:-2], refs[-2:]

    def step(i, totals):
        chi_total, hit_total = totals
        at = pl.ds(pl.multiple_of(i * WIDTH, WIDTH), WIDTH)
        cross, along, square = group_sums(genes, covs, part, left_ref, pieces, before, at)
        sumsq = square - jnp.sum(along * along, axis=0, keepdims=True)
        variance = jnp.maximum(sumsq, 0.0) / samples + VARIANCE_FLOOR
        zscore = cross * lax.rsqrt(variance * samples)
        chi = zscore * zscore
        hit = 1.0 / (1.0 + jnp.exp(8.0 - 2.0 * chi))
        for k in range(WIDTH // LANES):
            chi_total = chi_total + chi[:, k * LANES : (k + 1) * LANES]
            hit_total = hit_total + hit[:, k * LANES : (k + 1) * LANES]
        return chi_total, hit_total

    zeros = jnp.zeros((genes, LANES), jnp.float32)
    chi_ref[...], hit_ref[...] = lax.fori_loop(0, pieces[0].shape[1] // WIDTH, step, (zeros, zeros))


def call(body, shapes, left, pieces, before):
    vmem = pl.BlockSpec(memory_space=pltpu.VMEM)
    operands = [left, *pieces, *before]
    size = left.shape[1] * pieces[0].shape[1]
    return pl.pallas_call(
        functools.partial(body, len(pieces)),
        out_shape=tuple(jax.ShapeDtypeStruct(s, jnp.float32) for s in shapes),
        in_specs=[vmem] * len(operands),
        out_specs=(vmem,) * len(shapes),
        compiler_params=pltpu.CompilerParams(vmem_limit_bytes=VMEM_LIMIT),
        cost_estimate=pl.CostEstimate(flops=2 * left.shape[0] * size, bytes_accessed=2 * size, transcendentals=0),
    )(*operands)


def lay(*refs):
    start = 0
    for ref in refs[:-1]:
        refs[-1][start : start + ref.shape[0], :] = ref[...]
        start += ref.shape[0]


def packed_rows(pieces):
    vmem = pl.BlockSpec(memory_space=pltpu.VMEM)
    rows, width = sum(x.shape[0] for x in pieces), pieces[0].shape[1]
    return pl.pallas_call(
        lay,
        out_shape=jax.ShapeDtypeStruct((rows, width), pieces[0].dtype),
        in_specs=[vmem] * len(pieces),
        out_specs=vmem,
        compiler_params=pltpu.CompilerParams(vmem_limit_bytes=VMEM_LIMIT),
        cost_estimate=pl.CostEstimate(flops=rows * width, bytes_accessed=4 * rows * width, transcendentals=0),
    )(*pieces)


def groups(reach):
    edges = [0, *SWAPS]
    spans = list(zip(edges, edges[1:]))
    return [
        (range(a, reach + 1 if b == SWAPS[-1] else b), range(a + 1, b + 1)) for a, b in spans
    ]


def offsets(chips):
    order = []
    for keeps, gives in groups(chips // 2):
        order += [-k % chips for k in keeps] + [k % chips for k in gives]
    return order


def ordered(packed, z, core):
    chips = lax.axis_size("z")
    sign = 1 - 2 * core
    order = lax.rem(jnp.stack([z + sign * k for k in offsets(chips)]) + chips, chips)
    return packed.reshape(chips, -1, packed.shape[1])[order].reshape(packed.shape)


def turn(chips, value_ref, out_ref):
    rows = value_ref.shape[0] // chips
    order = offsets(chips)
    for i, k in enumerate(order):
        j = order.index(-k % chips)
        out_ref[i * rows : (i + 1) * rows, :] = value_ref[j * rows : (j + 1) * rows, :]


def turned(value, chips):
    vmem = pl.BlockSpec(memory_space=pltpu.VMEM)
    return pl.pallas_call(
        functools.partial(turn, chips),
        out_shape=jax.ShapeDtypeStruct(value.shape, value.dtype),
        in_specs=[vmem],
        out_specs=vmem,
        compiler_params=pltpu.CompilerParams(vmem_limit_bytes=VMEM_LIMIT),
        cost_estimate=pl.CostEstimate(flops=value.size, bytes_accessed=8 * value.size, transcendentals=0),
    )(value)


def residuals(basis, pheno, chips):
    resid = pheno - dot(basis, dot(basis, pheno, ((0,), (0,))), ((1,), (0,)))
    variance = jnp.mean(resid * resid, axis=0) + VARIANCE_FLOOR
    scaled = resid * lax.rsqrt(variance)[None, :]
    return jnp.stack(split(scaled.T, 2)), jnp.stack(split(turned(scaled, chips).T, 2))


def assembled(basis, terms):
    mine, sent = terms
    others = lax.ppermute(sent, "core", SWAP)
    return jnp.concatenate([mine[0], others[0], mine[1], others[1]] + split(basis.T, 3), axis=0)


def local(dosage, covars, phenotypes):
    chips = lax.axis_size("z")
    devices = chips * CORES
    rows, variants = dosage.shape
    covs = covars.shape[1]
    samples = rows * devices
    own = phenotypes.shape[1] // devices
    z = lax.axis_index("z")
    core = lax.axis_index("core")
    first = core == 0
    half = variants // CORES
    reach = chips // 2

    travel = [(2 * i, 2 * ((i + 1) % chips)) for i in range(chips)]
    travel += [(2 * i + 1, 2 * ((i - 1) % chips) + 1) for i in range(chips)]

    theirs = lax.ppermute(dosage, "core", SWAP)
    block = jnp.concatenate([jnp.where(first, dosage, theirs), jnp.where(first, theirs, dosage)], axis=0)
    part = half // PARTS
    keep = jnp.where(first, block[:, :half], block[:, half:])
    give = jnp.where(first, block[:, half:], block[:, :half])
    keep = [keep[:, i * part : (i + 1) * part] for i in range(PARTS)]
    give = [give[:, i * part : (i + 1) * part] for i in range(PARTS)]

    packed = jnp.concatenate(
        [phenotypes.reshape(rows, devices, own), jnp.broadcast_to(covars[:, None, :], (rows, devices, covs))], axis=2
    )
    packed = lax.all_to_all(packed, TILE, split_axis=1, concat_axis=0, tiled=True)
    packed = packed.reshape(samples, own + covs)

    kept, given = [keep], []
    swapped = []
    partial = [()] * PARTS
    genes = 2 * own

    def absorbed(index):
        keeps, gives = groups(reach)[index]
        size = (len(keeps) + len(gives)) * CORES * rows
        start = sum(len(x) + len(y) for x, y in groups(reach)[:index]) * CORES * rows
        used = left[:, start : start + size]
        last = index == len(SWAPS) - 1
        shapes = [(genes, LANES)] * 2 if last else [(genes, part), (covs, part), (1, part)]
        body = functools.partial(finish, samples) if last else absorb
        return [
            call(functools.partial(body, genes, covs, i), shapes, used, [kept[k][i] for k in keeps] + [swapped[index]], x)
            for i, x in enumerate(partial)
        ]

    for step in range(1, reach):
        held = give[-1]
        moved = []
        for value in keep + give:
            moved.append(lax.ppermute(value, TILE, travel))
        keep, give = moved[:PARTS], moved[PARTS:]
        kept.append(list(keep))
        given.append(give)
        if step in STAGES:
            packed, held = lax.optimization_barrier((packed, held))
        if step == STAGES[0]:
            keep[0], packed = lax.optimization_barrier((keep[0], ordered(packed, z, core)))
        if step == STAGES[1]:
            keep[0], basis = lax.optimization_barrier((keep[0], orthonormal(packed[:, own:])))
        if step == STAGES[2]:
            keep[0], basis = lax.optimization_barrier((keep[0], orthonormal(basis)))
        if step == STAGES[3]:
            keep[0], terms = lax.optimization_barrier((keep[0], residuals(basis, packed[:, :own], chips)))
        if step == STAGES[4]:
            keep[0], left = lax.optimization_barrier((keep[0], assembled(basis, terms)))
        if step in SWAPS:
            rows_given = packed_rows([x for y in zip(*given) for x in y])
            swapped.append(lax.ppermute(rows_given, "core", SWAP))
            given = []
        if step in ABSORBS:
            partial = absorbed(ABSORBS.index(step))
    for i, value in enumerate(keep):
        keep[i] = lax.ppermute(value, TILE, travel)
    kept.append(keep)
    chi, hit = (sum(x) for x in zip(*absorbed(len(SWAPS) - 1)))
    sums = jnp.stack([jnp.sum(chi, axis=1), jnp.sum(hit, axis=1)])
    sums = sums[:, :own] + lax.ppermute(sums[:, own:], "core", SWAP)
    return (sums[0] / variants, 20.0 / variants * sums[1])


def solution(mesh):
    cohorts, tiles = mesh.shape["cohort"], mesh.shape["tile"]
    finer = Mesh(mesh.devices.reshape(cohorts, tiles // CORES, CORES), AXES)
    return jax.shard_map(
        local,
        mesh=finer,
        in_specs=(P(AXES, None), P(AXES, None), P(AXES, None)),
        out_specs=(P(AXES), P(AXES)),
        check_vma=False,
    )
```
